32 devices in a mesh: branch: 16 (over z, y, core), head: 2 (over x).
Axes of the slice: x: 2, y: 2, z: 4, core: 2. Of those that a mesh axis runs over, the one named last changes fastest.
Arguments:
- queries: bfloat16 [16, 256, 64, 128], P('branch', None, 'head'), may hold values from -8 to 8
- grad_out: bfloat16 [16, 256, 64, 128], P('branch', None, 'head'), may hold values from -6 to 6
- branch_keys: bfloat16 [16, 256, 8, 128], P('branch', None, 'head'), may hold values from -8 to 8
- branch_values: bfloat16 [16, 256, 8, 128], P('branch', None, 'head'), may hold values from -6 to 6
- row_lse: float32 [16, 64, 256], P('branch', 'head'), may hold values from -100 to 100, as said below
- row_delta: float32 [16, 64, 256], P('branch', 'head'), may hold values from -36 to 36
- lengths: int32 [16], P('branch'), may hold values from 128 to 256, as said below
- prompt_keys: bfloat16 [512, 8, 128], P(('branch', 'head')), may hold values from -8 to 8
- prompt_values: bfloat16 [512, 8, 128], P(('branch', 'head')), may hold values from -6 to 6
Outputs:
- query_grads: bfloat16 [16, 256, 64, 128], P('branch', None, 'head')
- branch_dkey: bfloat16 [16, 256, 8, 128], P('branch', None, 'head')
- branch_dvalue: bfloat16 [16, 256, 8, 128], P('branch', None, 'head')
- prompt_dkey: bfloat16 [512, 8, 128], P(('branch', 'head'))
- prompt_dvalue: bfloat16 [512, 8, 128], P(('branch', 'head'))
The draws below stay inside these ranges and needn't reach their ends.
Inputs may be any that keep to these rules, and one draw needn't show every extreme that they name: row_lse[b, h, i] is the logarithm of the sum of exp(scaling * queries[b, i, h] . K_b[t, group of h]) over all t < 512 + i + 1, whatever the branch's length. `lengths`: some branch has exactly 256 valid positions and some exactly 128.
All inputs are finite; a program needn't handle non-finite values.
Results may differ from the reference program's by a relative error of at most 0.008.
Values may be sent and summed in bfloat16 or wider, within the bound.
A program may use at most 64 MiB of HBM per device.

```python
import math
import jax
import jax.numpy as jnp
from jax import lax

HEADS = 64
KVG = 8
HD = 128
SUF = 256
PRE = 512
BRANCHES = 16


def make_queries(key):
    first = jax.random.fold_in(key, 101)
    return jax.random.normal(first, (BRANCHES, SUF, HEADS, HD), jnp.float32).astype(jnp.bfloat16)


def make_branch_keys(key):
    return jax.random.normal(jax.random.fold_in(key, 201), (BRANCHES, SUF, KVG, HD), jnp.float32).astype(jnp.bfloat16)


def make_prompt_keys(key):
    return jax.random.normal(jax.random.fold_in(key, 202), (PRE, KVG, HD), jnp.float32).astype(jnp.bfloat16)


def draw_queries(key, part):
    return make_queries(key)


def draw_branch_keys(key, part):
    return make_branch_keys(key)


def draw_prompt_keys(key, part):
    return make_prompt_keys(key)


def draw_row_lse(key, part):
    queries = make_queries(key).astype(jnp.float32)
    branch_keys = make_branch_keys(key).astype(jnp.float32)
    prompt_keys = make_prompt_keys(key).astype(jnp.float32)
    scaling = 1.0 / math.sqrt(HD)
    group_size = HEADS // KVG
    positions = jnp.arange(SUF, dtype=jnp.int32)
    key_positions = jnp.arange(PRE + SUF, dtype=jnp.int32) - PRE
    visible = key_positions[None, :] <= positions[:, None]

    def per_branch(branch_items):
        query_b, keys_b = branch_items
        key_rows = jnp.concatenate([prompt_keys, keys_b], 0)
        scores = jnp.einsum('sgrd,kgd->grsk', query_b.reshape(SUF, KVG, group_size, HD), key_rows) * scaling
        scores = jnp.where(visible, scores, -1e+30)
        return jax.nn.logsumexp(scores, axis=-1).reshape(HEADS, SUF)
    return lax.map(per_branch, (queries, branch_keys)).astype(jnp.float32)


def draw_lengths(key, part):
    base = jax.random.randint(jax.random.fold_in(key, 301), (BRANCHES,), SUF // 2, SUF + 1).astype(jnp.int32)
    order = jax.random.permutation(jax.random.fold_in(key, 302), BRANCHES)
    base = base.at[order[0]].set(SUF)
    base = base.at[order[1]].set(SUF // 2)
    return base.astype(jnp.int32)


def levels(own_key, extent, pieces, smallest, top_value):
    def one(position, parts):
        draws = jax.random.uniform(jax.random.fold_in(jax.random.fold_in(own_key, 6), position), (parts,), jnp.float32, smallest / len(pieces), top_value / len(pieces))
        return jnp.repeat(jnp.exp(draws), extent[position] // parts).reshape((-1,) + (1,) * (len(extent) - position - 1))

    gain = one(*pieces[0])
    for cut in pieces[1:]:
        gain = gain * one(*cut)
    return gain


def noise(own_key, shape, scale, most, shards=(), held_as=jnp.bfloat16):
    factor_of = levels(own_key, shape, shards, -0.22, 0.18) if shards else 1.0
    result = jax.random.normal(own_key, shape, jnp.float32) * scale * factor_of
    return jnp.minimum(jnp.maximum(result, -most), most).astype(held_as)


def setup_inputs(seed: int = 0) -> dict:
    keys = jax.random.split(jax.random.key(seed), 10)
    return {
        "queries": draw_queries(jax.random.fold_in(keys[9], 71), 0),
        "grad_out": noise(keys[1], (BRANCHES, SUF, HEADS, HD), 1.0, 6.0, ((0, 16), (2, 2))),
        "branch_keys": draw_branch_keys(jax.random.fold_in(keys[9], 71), 0),
        "branch_values": noise(keys[3], (BRANCHES, SUF, KVG, HD), 1.0, 6.0, ((0, 16), (2, 2))),
        "row_lse": draw_row_lse(jax.random.fold_in(keys[9], 71), 0),
        "row_delta": noise(keys[5], (BRANCHES, HEADS, SUF), 6.0, 36.0, ((0, 16), (1, 2)), jnp.float32),
        "lengths": draw_lengths(jax.random.fold_in(keys[9], 71), 0),
        "prompt_keys": draw_prompt_keys(jax.random.fold_in(keys[9], 71), 0),
        "prompt_values": noise(keys[8], (PRE, KVG, HD), 1.0, 6.0, ((0, 32),)),
    }


def block_grads(queries, grad_out, lse_rows, delta_rows, key_rows, value_rows, visible, scaling):
    query_float = queries.astype(jnp.float32)
    grad_float = grad_out.astype(jnp.float32)
    key_float = key_rows.astype(jnp.float32)
    value_float = value_rows.astype(jnp.float32)
    scores = jnp.einsum('sgrd,kgd->grsk', query_float, key_float) * scaling
    weights = jnp.where(visible, jnp.exp(scores - lse_rows[..., None]), 0.0)
    weights_low = lax.optimization_barrier(weights.astype(jnp.bfloat16)).astype(jnp.float32)
    value_grad = jnp.einsum('grsk,sgrd->kgd', weights_low, grad_float)
    weight_grad = jnp.einsum('sgrd,kgd->grsk', grad_float, value_float)
    score_grad = lax.optimization_barrier((weights * (weight_grad - delta_rows[..., None])).astype(jnp.bfloat16)).astype(jnp.float32)
    query_grad = jnp.einsum('grsk,kgd->sgrd', score_grad, key_float) * scaling
    key_grad = jnp.einsum('grsk,sgrd->kgd', score_grad, query_float) * scaling
    return (query_grad, key_grad, value_grad)

def reference(queries, grad_out, branch_keys, branch_values, row_lse, row_delta, lengths, prompt_keys, prompt_values):
    seq_len = queries.shape[1]
    head_count = queries.shape[2]
    head_dim = queries.shape[3]
    groups = branch_keys.shape[2]
    group_size = head_count // groups
    prompt_len = prompt_keys.shape[0]
    scaling = 1.0 / math.sqrt(head_dim)
    positions = jnp.arange(seq_len, dtype=jnp.int32)
    key_positions = jnp.arange(prompt_len + seq_len, dtype=jnp.int32) - prompt_len

    def per_branch(running, branch_items):
        query_b, grad_b, keys_b, values_b, lse_b, delta_b, length = branch_items
        key_rows = jnp.concatenate([prompt_keys, keys_b], 0)
        value_rows = jnp.concatenate([prompt_values, values_b], 0)
        live_rows = positions < length
        visible = live_rows[:, None] & (key_positions[None, :] <= positions[:, None])
        query_grad, key_grad, value_grad = block_grads(query_b.reshape(seq_len, groups, group_size, head_dim), grad_b.reshape(seq_len, groups, group_size, head_dim), lse_b.reshape(groups, group_size, seq_len), delta_b.reshape(groups, group_size, seq_len), key_rows, value_rows, visible, scaling)
        running = (running[0] + key_grad[:prompt_len], running[1] + value_grad[:prompt_len])
        results = (query_grad.reshape(seq_len, head_count, head_dim).astype(jnp.bfloat16), key_grad[prompt_len:].astype(jnp.bfloat16), value_grad[prompt_len:].astype(jnp.bfloat16))
        return (running, results)
    start = (jnp.zeros((prompt_len, groups, head_dim), jnp.float32), jnp.zeros((prompt_len, groups, head_dim), jnp.float32))
    totals, results = lax.scan(per_branch, start, (queries, grad_out, branch_keys, branch_values, row_lse, row_delta, lengths))
    return (results[0], results[1], results[2], totals[0].astype(jnp.bfloat16), totals[1].astype(jnp.bfloat16))
```

```python
import functools
import math

import jax
import jax.numpy as jnp
from jax import lax
from jax.experimental import pallas as pl
from jax.experimental.pallas import tpu as pltpu
from jax.sharding import PartitionSpec as P


def score_pieces(queries, grad_out, lse_rows, delta_rows, key_rows, value_rows, visible, scaling):
    scores = (
        jnp.einsum("sgrd,kgd->grsk", queries, key_rows, preferred_element_type=jnp.float32)
        * scaling
    )
    weights = jnp.where(visible, jnp.exp(scores - lse_rows[..., None]), 0.0)
    weights_low = weights.astype(jnp.bfloat16)
    weight_grad = jnp.einsum(
        "sgrd,kgd->grsk", grad_out, value_rows, preferred_element_type=jnp.float32
    )
    score_grad = (weights * (weight_grad - delta_rows[..., None])).astype(jnp.bfloat16)
    query_grad = (
        jnp.einsum("grsk,kgd->sgrd", score_grad, key_rows, preferred_element_type=jnp.float32)
        * scaling
    )
    return (query_grad, weights_low, score_grad)


def edge_grads(weights_low, score_grad, queries, grad_out, scaling):
    value_grad = jnp.einsum(
        "grsk,sgrd->kgd", weights_low, grad_out, preferred_element_type=jnp.float32
    )
    key_grad = (
        jnp.einsum("grsk,sgrd->kgd", score_grad, queries, preferred_element_type=jnp.float32)
        * scaling
    )
    return (key_grad, value_grad)


def block_size():
    return 256


def regroup(rows, outer, inner):
    shaped = rows.reshape((outer, inner, rows.shape[0] // (outer * inner)) + rows.shape[1:])
    return jnp.swapaxes(shaped, 0, 1).reshape(rows.shape)


def plain_shards(
    queries,
    grad_out,
    branch_keys,
    branch_values,
    row_lse,
    row_delta,
    lengths,
    prompt_keys,
    prompt_values,
):
    seq_len = queries.shape[1]
    head_count = queries.shape[2]
    head_dim = queries.shape[3]
    groups = branch_keys.shape[2]
    group_size = head_count // groups
    scaling = 1.0 / math.sqrt(head_dim)
    branch_count = lax.axis_size("branch")
    head_devices = lax.axis_size("head")
    query_grouped = queries[0].reshape(seq_len, groups, group_size, head_dim)
    grad_grouped = grad_out[0].reshape(seq_len, groups, group_size, head_dim)
    lse_rows = row_lse[0].reshape(groups, group_size, seq_len)
    delta_rows = row_delta[0].reshape(groups, group_size, seq_len)
    positions = lax.iota(jnp.int32, seq_len)
    live_rows = positions < lengths[0]
    wide_keys, wide_values = (
        lax.all_gather(prompt_keys, "branch", axis=0, tiled=True),
        lax.all_gather(prompt_values, "branch", axis=0, tiled=True),
    )
    mixed_keys, mixed_values = (
        lax.all_to_all(wide_keys, "head", split_axis=1, concat_axis=0, tiled=True),
        lax.all_to_all(wide_values, "head", split_axis=1, concat_axis=0, tiled=True),
    )
    cache_keys = regroup(mixed_keys, head_devices, branch_count)
    cache_values = regroup(mixed_values, head_devices, branch_count)
    query_total = jnp.zeros((seq_len, groups, group_size, head_dim), jnp.float32)
    prompt_len = cache_keys.shape[0]
    prompt_block = block_size()
    prompt_visible = live_rows[:, None]
    low_parts = []
    grad_parts = []
    for offset in range(0, prompt_len, prompt_block):
        query_part, weights_low, score_grad = score_pieces(
            query_grouped,
            grad_grouped,
            lse_rows,
            delta_rows,
            cache_keys[offset : offset + prompt_block],
            cache_values[offset : offset + prompt_block],
            prompt_visible,
            scaling,
        )
        query_total = query_total + query_part
        low_parts.append(weights_low)
        grad_parts.append(score_grad)
    branch_block = block_size()
    offset = 0
    key_positions = offset + lax.iota(jnp.int32, branch_block)
    visible = live_rows[:, None] & (key_positions[None, :] <= positions[:, None])
    query_part, weights_low, score_grad = score_pieces(
        query_grouped,
        grad_grouped,
        lse_rows,
        delta_rows,
        branch_keys[0, offset : offset + branch_block],
        branch_values[0, offset : offset + branch_block],
        visible,
        scaling,
    )
    key_part, value_part = edge_grads(weights_low, score_grad, query_grouped, grad_grouped, scaling)
    query_total = query_total + query_part
    own_dkey = key_part.astype(jnp.bfloat16)
    own_dvalue = value_part.astype(jnp.bfloat16)
    stored_low = jnp.concatenate(low_parts, 3)
    stored_grad = jnp.concatenate(grad_parts, 3)
    key_term, value_term = edge_grads(stored_low, stored_grad, query_grouped, grad_grouped, scaling)
    summed = lax.psum_scatter(
        jnp.stack([key_term, value_term], 1), "branch", scatter_dimension=0, tiled=True
    )
    prompt_dkey, prompt_dvalue = (
        lax.all_to_all(
            summed[:, 0].astype(jnp.bfloat16), "head", split_axis=0, concat_axis=1, tiled=True
        ),
        lax.all_to_all(
            summed[:, 1].astype(jnp.bfloat16), "head", split_axis=0, concat_axis=1, tiled=True
        ),
    )
    query_grads = query_total.reshape(seq_len, head_count, head_dim).astype(jnp.bfloat16)[None]
    branch_dkey = own_dkey[None]
    branch_dvalue = own_dvalue[None]
    return (query_grads, branch_dkey, branch_dvalue, prompt_dkey, prompt_dvalue)


MESH = pl.DeviceIdType.MESH
LOG2E = math.log2(math.e)
NT = (((1,), (1,)), ((), ()))


def block_terms(q, do, lse, delta, k, v, k_t, keep, score_scale):
    s = lax.dot_general(k, q, NT, preferred_element_type=jnp.float32)
    p = jnp.exp2(s * score_scale - lse)
    if keep is not None:
        p = jnp.where(keep, p, 0.0)
    dp = lax.dot_general(v, do, NT, preferred_element_type=jnp.float32)
    ds = (p * (dp - delta)).astype(jnp.bfloat16)
    dv = jnp.dot(p.astype(jnp.bfloat16), do, preferred_element_type=jnp.float32)
    dk = jnp.dot(ds, q, preferred_element_type=jnp.float32)
    dq_t = jnp.dot(k_t, ds, preferred_element_type=jnp.float32)
    return dq_t, dk, dv


def fused_kernel(
    dims,
    q_hbm,
    do_hbm,
    bk_ref,
    bv_ref,
    rows_ref,
    packed_ref,
    dq_hbm,
    bdk_ref,
    bdv_ref,
    pd_ref,
    q_scr,
    do_scr,
    dq_acc,
    dq_scr,
    dk_acc,
    dv_acc,
    kt_scr,
    gath,
    send,
    recv,
    load_sem,
    store_sem,
    gather_sem,
    own_sem,
    scatter_send_sem,
    scatter_recv_sem,
):
    branch_count, head_devices, groups, group_size, seq_len, head_dim, pos = dims
    devices = branch_count * head_devices
    prompt_len = devices * pos
    scaling = 1.0 / math.sqrt(head_dim)
    score_scale = scaling * LOG2E
    rows = seq_len * group_size
    wide = 64 * group_size
    chunk = 256
    early = groups // 2
    me = lax.axis_index("branch") * head_devices + lax.axis_index("head")

    def ident(index):
        return (index // head_devices, index % head_devices)

    def loads(g):
        cut = pl.ds(g * group_size, group_size)
        return (
            pltpu.make_async_copy(q_hbm.at[0, :, cut, :], q_scr.at[g], load_sem.at[0, g]),
            pltpu.make_async_copy(do_hbm.at[0, :, cut, :], do_scr.at[g], load_sem.at[1, g]),
        )

    for g in range(groups):
        for copy in loads(g):
            copy.start()

    barrier = pltpu.get_barrier_semaphore()

    @pl.loop(1, devices)
    def _(k):
        pl.semaphore_signal(
            barrier, inc=1, device_id=ident((me + k) % devices), device_id_type=MESH
        )

    dq_acc[...] = jnp.zeros_like(dq_acc)
    pl.semaphore_wait(barrier, devices - 1)

    @pl.loop(1, devices)
    def _(k):
        other = (me + k) % devices
        pltpu.make_async_remote_copy(
            src_ref=packed_ref.at[other % head_devices],
            dst_ref=gath.at[k],
            send_sem=gather_sem.at[0],
            recv_sem=gather_sem.at[1],
            device_id=ident(other),
            device_id_type=MESH,
        ).start()

    own = pltpu.make_async_copy(packed_ref.at[me % head_devices], gath.at[0], own_sem)
    own.start()

    def row_block(g, j):
        cut = pl.ds(j * 64, 64)
        q = q_scr[g, cut].reshape(wide, head_dim)
        do = do_scr[g, cut].reshape(wide, head_dim)
        return q, do, rows_ref[g, j, 0:1, :], rows_ref[g, j, 1:2, :]

    def branch_part(g):
        k_all = bk_ref[g]
        v_all = bv_ref[g]
        k_t_all = k_all.T
        steps = seq_len // 64
        for j in reversed(range(steps)):
            seen = (j + 1) * 64
            q, do, lse, delta = row_block(g, j)
            key_at = lax.broadcasted_iota(jnp.int32, (seen, wide), 0)
            row_at = lax.broadcasted_iota(jnp.int32, (seen, wide), 1) // group_size
            dq_t, dk, dv = block_terms(
                q, do, lse, delta, k_all[:seen], v_all[:seen], k_t_all[:, :seen],
                key_at <= row_at + j * 64, score_scale,
            )
            dq_acc[g, j] += dq_t
            if j == steps - 1:
                dk_acc[0:seen] = dk
                dv_acc[0:seen] = dv
            else:
                dk_acc[0:seen] += dk
                dv_acc[0:seen] += dv
        bdk_ref[g] = (dk_acc[0:seq_len] * scaling).astype(jnp.bfloat16)
        bdv_ref[g] = dv_acc[0:seq_len].astype(jnp.bfloat16)

    def prompt_part(g):
        kt_scr[...] = gath[:, 0, g].reshape(prompt_len, head_dim).T
        dk_acc[...] = jnp.zeros_like(dk_acc)
        dv_acc[...] = jnp.zeros_like(dv_acc)
        per = chunk // pos

        @pl.loop(0, seq_len // 64)
        def _(j):
            q, do, lse, delta = row_block(g, j)
            total = None
            for c in range(prompt_len // chunk):
                at = slice(c * chunk, (c + 1) * chunk)
                k = gath[c * per : (c + 1) * per, 0, g].reshape(chunk, head_dim)
                v = gath[c * per : (c + 1) * per, 1, g].reshape(chunk, head_dim)
                dq_t, dk, dv = block_terms(
                    q, do, lse, delta, k, v, kt_scr[:, at], None, score_scale
                )
                dk_acc[at] += dk
                dv_acc[at] += dv
                total = dq_t if total is None else total + dq_t
            dq_acc[g, j] += total

        send[g, :, 0] = (dk_acc[...] * scaling).astype(jnp.bfloat16).reshape(devices, pos, head_dim)
        send[g, :, 1] = dv_acc[...].astype(jnp.bfloat16).reshape(devices, pos, head_dim)

        @pl.loop(1, devices)
        def _(k):
            pltpu.make_async_remote_copy(
                src_ref=send.at[g, k],
                dst_ref=recv.at[g, k],
                send_sem=scatter_send_sem.at[g],
                recv_sem=scatter_recv_sem.at[g],
                device_id=ident((me + devices - k) % devices),
                device_id_type=MESH,
            ).start()

    def store(g):
        cut = pl.ds(g * group_size, group_size)
        return pltpu.make_async_copy(dq_scr.at[g], dq_hbm.at[0, :, cut, :], store_sem.at[g])

    def finish(g):
        for j in range(seq_len // 64):
            dq_scr[g, j * 64 : (j + 1) * 64] = (
                (dq_acc[g, j] * scaling).T.astype(jnp.bfloat16).reshape(64, group_size, head_dim)
            )
        store(g).start()

    @pl.loop(0, early)
    def _(g):
        for copy in loads(g):
            copy.wait()
        branch_part(g)

    own.wait()
    rest = pl.ds(1, devices - 1)
    pltpu.make_async_copy(gath.at[rest], gath.at[rest], gather_sem.at[1]).wait()

    @pl.loop(0, groups)
    def _(g):
        @pl.when(g >= early)
        def _():
            for copy in loads(g):
                copy.wait()

        prompt_part(g)

    @pl.loop(0, early)
    def _(g):
        finish(g)

    @pl.loop(early, groups)
    def _(g):
        branch_part(g)
        finish(g)

    pltpu.make_async_copy(gath.at[rest], gath.at[rest], gather_sem.at[0]).wait()

    @pl.loop(0, groups)
    def _(g):
        pltpu.make_async_copy(send.at[g, rest], send.at[g, rest], scatter_send_sem.at[g]).wait()
        pltpu.make_async_copy(recv.at[g, rest], recv.at[g, rest], scatter_recv_sem.at[g]).wait()
        for apart in range(head_devices):
            owner = (me + apart) % head_devices
            total = None
            for k in range(apart, devices, head_devices):
                piece = (send if k == 0 else recv)[g, k].astype(jnp.float32)
                total = piece if total is None else total + piece
            pd_ref[owner, g] = total.astype(jnp.bfloat16)
        store(g).wait()


def shards(
    queries,
    grad_out,
    branch_keys,
    branch_values,
    row_lse,
    row_delta,
    lengths,
    prompt_keys,
    prompt_values,
):
    branch_count = lax.axis_size("branch")
    head_devices = lax.axis_size("head")
    devices = branch_count * head_devices
    _, seq_len, head_count, head_dim = queries.shape
    groups = branch_keys.shape[2]
    group_size = head_count // groups
    pos = prompt_keys.shape[0]
    if pos % 16:
        return plain_shards(
            queries, grad_out, branch_keys, branch_values, row_lse, row_delta, lengths,
            prompt_keys, prompt_values,
        )
    prompt_len = devices * pos
    wide = 64 * group_size
    steps = seq_len // 64
    live = lax.iota(jnp.int32, seq_len) < lengths[0]
    lse = jnp.where(live, row_lse[0] * LOG2E, 1e30)
    rows = jnp.stack([lse, row_delta[0]])
    rows = rows.reshape(2, groups, group_size, steps, 64)
    rows = rows.transpose(1, 3, 0, 4, 2).reshape(groups, steps, 2, wide)
    packed = jnp.stack([prompt_keys, prompt_values])
    packed = packed.reshape(2, pos, head_devices, groups, head_dim).transpose(2, 0, 3, 1, 4)
    dims = (branch_count, head_devices, groups, group_size, seq_len, head_dim, pos)
    vmem = pl.BlockSpec(memory_space=pltpu.VMEM)
    hbm = pl.BlockSpec(memory_space=pl.ANY)
    low, full = jnp.bfloat16, jnp.float32
    dq, bdk, bdv, pd = pl.pallas_call(
        functools.partial(fused_kernel, dims),
        out_shape=(
            jax.ShapeDtypeStruct(queries.shape, low),
            jax.ShapeDtypeStruct((groups, seq_len, head_dim), low),
            jax.ShapeDtypeStruct((groups, seq_len, head_dim), low),
            jax.ShapeDtypeStruct((head_devices, groups, 2, pos, head_dim), low),
        ),
        in_specs=[hbm, hbm, vmem, vmem, vmem, vmem],
        out_specs=(hbm, vmem, vmem, vmem),
        scratch_shapes=[
            pltpu.VMEM((groups, seq_len, group_size, head_dim), low),
            pltpu.VMEM((groups, seq_len, group_size, head_dim), low),
            pltpu.VMEM((groups, steps, head_dim, wide), full),
            pltpu.VMEM((groups, seq_len, group_size, head_dim), low),
            pltpu.VMEM((prompt_len, head_dim), full),
            pltpu.VMEM((prompt_len, head_dim), full),
            pltpu.VMEM((head_dim, prompt_len), low),
            pltpu.VMEM((devices, 2, groups, pos, head_dim), low),
            pltpu.VMEM((groups, devices, 2, pos, head_dim), low),
            pltpu.VMEM((groups, devices, 2, pos, head_dim), low),
            pltpu.SemaphoreType.DMA((2, groups)),
            pltpu.SemaphoreType.DMA((groups,)),
            pltpu.SemaphoreType.DMA((2,)),
            pltpu.SemaphoreType.DMA,
            pltpu.SemaphoreType.DMA((groups,)),
            pltpu.SemaphoreType.DMA((groups,)),
        ],
        compiler_params=pltpu.CompilerParams(collective_id=0, has_side_effects=True),
    )(
        queries,
        grad_out,
        branch_keys[0].swapaxes(0, 1),
        branch_values[0].swapaxes(0, 1),
        rows,
        packed,
    )
    pd = pd.transpose(2, 3, 0, 1, 4).reshape(2, pos, head_devices * groups, head_dim)
    return (dq, bdk.swapaxes(0, 1)[None], bdv.swapaxes(0, 1)[None], pd[0], pd[1])


def solution(mesh):
    in_specs = (
        P("branch", None, "head", None),
        P("branch", None, "head", None),
        P("branch", None, "head", None),
        P("branch", None, "head", None),
        P("branch", "head", None),
        P("branch", "head", None),
        P("branch"),
        P(("branch", "head"), None, None),
        P(("branch", "head"), None, None),
    )
    out_specs = (
        P("branch", None, "head", None),
        P("branch", None, "head", None),
        P("branch", None, "head", None),
        P(("branch", "head"), None, None),
        P(("branch", "head"), None, None),
    )
    return jax.shard_map(shards, mesh=mesh, in_specs=in_specs, out_specs=out_specs, check_vma=False)
```

```python
import functools
import math

import jax
import jax.numpy as jnp
from jax import lax
from jax.experimental import pallas as pl
from jax.experimental.pallas import tpu as pltpu
from jax.sharding import PartitionSpec as P


def score_pieces(queries, grad_out, lse_rows, delta_rows, key_rows, value_rows, visible, scaling):
    scores = (
        jnp.einsum("sgrd,kgd->grsk", queries, key_rows, preferred_element_type=jnp.float32)
        * scaling
    )
    weights = jnp.where(visible, jnp.exp(scores - lse_rows[..., None]), 0.0)
    weights_low = weights.astype(jnp.bfloat16)
    weight_grad = jnp.einsum(
        "sgrd,kgd->grsk", grad_out, value_rows, preferred_element_type=jnp.float32
    )
    score_grad = (weights * (weight_grad - delta_rows[..., None])).astype(jnp.bfloat16)
    query_grad = (
        jnp.einsum("grsk,kgd->sgrd", score_grad, key_rows, preferred_element_type=jnp.float32)
        * scaling
    )
    return (query_grad, weights_low, score_grad)


def edge_grads(weights_low, score_grad, queries, grad_out, scaling):
    value_grad = jnp.einsum(
        "grsk,sgrd->kgd", weights_low, grad_out, preferred_element_type=jnp.float32
    )
    key_grad = (
        jnp.einsum("grsk,sgrd->kgd", score_grad, queries, preferred_element_type=jnp.float32)
        * scaling
    )
    return (key_grad, value_grad)


def block_size():
    return 256


def regroup(rows, outer, inner):
    shaped = rows.reshape((outer, inner, rows.shape[0] // (outer * inner)) + rows.shape[1:])
    return jnp.swapaxes(shaped, 0, 1).reshape(rows.shape)


def plain_shards(
    queries,
    grad_out,
    branch_keys,
    branch_values,
    row_lse,
    row_delta,
    lengths,
    prompt_keys,
    prompt_values,
):
    seq_len = queries.shape[1]
    head_count = queries.shape[2]
    head_dim = queries.shape[3]
    groups = branch_keys.shape[2]
    group_size = head_count // groups
    scaling = 1.0 / math.sqrt(head_dim)
    branch_count = lax.axis_size("branch")
    head_devices = lax.axis_size("head")
    query_grouped = queries[0].reshape(seq_len, groups, group_size, head_dim)
    grad_grouped = grad_out[0].reshape(seq_len, groups, group_size, head_dim)
    lse_rows = row_lse[0].reshape(groups, group_size, seq_len)
    delta_rows = row_delta[0].reshape(groups, group_size, seq_len)
    positions = lax.iota(jnp.int32, seq_len)
    live_rows = positions < lengths[0]
    wide_keys, wide_values = (
        lax.all_gather(prompt_keys, "branch", axis=0, tiled=True),
        lax.all_gather(prompt_values, "branch", axis=0, tiled=True),
    )
    mixed_keys, mixed_values = (
        lax.all_to_all(wide_keys, "head", split_axis=1, concat_axis=0, tiled=True),
        lax.all_to_all(wide_values, "head", split_axis=1, concat_axis=0, tiled=True),
    )
    cache_keys = regroup(mixed_keys, head_devices, branch_count)
    cache_values = regroup(mixed_values, head_devices, branch_count)
    query_total = jnp.zeros((seq_len, groups, group_size, head_dim), jnp.float32)
    prompt_len = cache_keys.shape[0]
    prompt_block = block_size()
    prompt_visible = live_rows[:, None]
    low_parts = []
    grad_parts = []
    for offset in range(0, prompt_len, prompt_block):
        query_part, weights_low, score_grad = score_pieces(
            query_grouped,
            grad_grouped,
            lse_rows,
            delta_rows,
            cache_keys[offset : offset + prompt_block],
            cache_values[offset : offset + prompt_block],
            prompt_visible,
            scaling,
        )
        query_total = query_total + query_part
        low_parts.append(weights_low)
        grad_parts.append(score_grad)
    branch_block = block_size()
    offset = 0
    key_positions = offset + lax.iota(jnp.int32, branch_block)
    visible = live_rows[:, None] & (key_positions[None, :] <= positions[:, None])
    query_part, weights_low, score_grad = score_pieces(
        query_grouped,
        grad_grouped,
        lse_rows,
        delta_rows,
        branch_keys[0, offset : offset + branch_block],
        branch_values[0, offset : offset + branch_block],
        visible,
        scaling,
    )
    key_part, value_part = edge_grads(weights_low, score_grad, query_grouped, grad_grouped, scaling)
    query_total = query_total + query_part
    own_dkey = key_part.astype(jnp.bfloat16)
    own_dvalue = value_part.astype(jnp.bfloat16)
    stored_low = jnp.concatenate(low_parts, 3)
    stored_grad = jnp.concatenate(grad_parts, 3)
    key_term, value_term = edge_grads(stored_low, stored_grad, query_grouped, grad_grouped, scaling)
    summed = lax.psum_scatter(
        jnp.stack([key_term, value_term], 1), "branch", scatter_dimension=0, tiled=True
    )
    prompt_dkey, prompt_dvalue = (
        lax.all_to_all(
            summed[:, 0].astype(jnp.bfloat16), "head", split_axis=0, concat_axis=1, tiled=True
        ),
        lax.all_to_all(
            summed[:, 1].astype(jnp.bfloat16), "head", split_axis=0, concat_axis=1, tiled=True
        ),
    )
    query_grads = query_total.reshape(seq_len, head_count, head_dim).astype(jnp.bfloat16)[None]
    branch_dkey = own_dkey[None]
    branch_dvalue = own_dvalue[None]
    return (query_grads, branch_dkey, branch_dvalue, prompt_dkey, prompt_dvalue)


MESH = pl.DeviceIdType.MESH
LOG2E = math.log2(math.e)
NT = (((1,), (1,)), ((), ()))


def block_terms(q, do, lse, delta, k, v, k_t, keep, score_scale):
    s = lax.dot_general(k, q, NT, preferred_element_type=jnp.float32)
    p = jnp.exp2(s * score_scale - lse)
    if keep is not None:
        p = jnp.where(keep, p, 0.0)
    dp = lax.dot_general(v, do, NT, preferred_element_type=jnp.float32)
    ds = (p * (dp - delta)).astype(jnp.bfloat16)
    dv = jnp.dot(p.astype(jnp.bfloat16), do, preferred_element_type=jnp.float32)
    dk = jnp.dot(ds, q, preferred_element_type=jnp.float32)
    dq_t = jnp.dot(k_t, ds, preferred_element_type=jnp.float32)
    return dq_t, dk, dv


def fused_kernel(
    dims,
    q_hbm,
    do_hbm,
    bk_ref,
    bv_ref,
    rows_ref,
    packed_ref,
    dq_hbm,
    bdk_ref,
    bdv_ref,
    pd_ref,
    q_scr,
    do_scr,
    dq_acc,
    dq_scr,
    dk_acc,
    dv_acc,
    kt_scr,
    gath,
    own_part,
    send,
    half,
    comb,
    recv,
    load_sem,
    store_sem,
    own_sem,
    gather_sem,
    pass_sem,
    half_sem,
    scatter_sem,
):
    branch_count, head_devices, groups, group_size, seq_len, head_dim, pos = dims
    devices = branch_count * head_devices
    prompt_len = devices * pos
    scaling = 1.0 / math.sqrt(head_dim)
    score_scale = scaling * LOG2E
    rows = seq_len * group_size
    wide = 64 * group_size
    chunk = prompt_len // 2
    early = groups // 2
    chips = branch_count // 2 * head_devices
    core = lax.axis_index("branch") % 2
    me = lax.axis_index("branch") // 2 * head_devices + lax.axis_index("head")
    partner = (lax.axis_index("branch") + 1 - 2 * core, lax.axis_index("head"))
    far = pl.ds(1, chips - 1)

    def peer(chip):
        return (chip // head_devices * 2 + core, chip % head_devices)

    def wait_bytes(ref, sem):
        pltpu.make_async_copy(ref, ref, sem).wait()

    def loads(g):
        cut = pl.ds(g * group_size, group_size)
        return (
            pltpu.make_async_copy(q_hbm.at[0, :, cut, :], q_scr.at[g], load_sem.at[0, g]),
            pltpu.make_async_copy(do_hbm.at[0, :, cut, :], do_scr.at[g], load_sem.at[1, g]),
        )

    for g in range(groups):
        for copy in loads(g):
            copy.start()

    barrier = pltpu.get_barrier_semaphore()

    @pl.loop(1, chips)
    def _(k):
        pl.semaphore_signal(
            barrier, inc=1, device_id=peer((me + k) % chips), device_id_type=MESH
        )

    pl.semaphore_signal(barrier, inc=1, device_id=partner, device_id_type=MESH)

    def own_copy(g):
        return pltpu.make_async_copy(
            packed_ref.at[me % head_devices, g], gath.at[g, 0, 0], own_sem.at[g]
        )

    for g in range(groups):
        own_copy(g).start()
    dq_acc[...] = jnp.zeros_like(dq_acc)
    pl.semaphore_wait(barrier, chips)

    @pl.loop(0, groups)
    def _(g):
        @pl.loop(1, chips)
        def _(k):
            other = (me + k) % chips
            pltpu.make_async_remote_copy(
                src_ref=packed_ref.at[other % head_devices, g],
                dst_ref=gath.at[g, 0, k],
                send_sem=gather_sem.at[0, g],
                recv_sem=gather_sem.at[1, g],
                device_id=peer(other),
                device_id_type=MESH,
            ).start()

    def pass_copy(g):
        return pltpu.make_async_remote_copy(
            src_ref=gath.at[g, 0],
            dst_ref=gath.at[g, 1],
            send_sem=pass_sem.at[0, g],
            recv_sem=pass_sem.at[1, g],
            device_id=partner,
            device_id_type=MESH,
        )

    def pass_on(g):
        own_copy(g).wait()
        wait_bytes(gath.at[g, 0, far], gather_sem.at[1, g])
        pass_copy(g).start()

    def half_copy(g):
        return pltpu.make_async_remote_copy(
            src_ref=send.at[g],
            dst_ref=half.at[g],
            send_sem=half_sem.at[0, g],
            recv_sem=half_sem.at[1, g],
            device_id=partner,
            device_id_type=MESH,
        )

    def combine(g):
        half_copy(g).wait_recv()
        comb[g] = (own_part[g] + half[g].astype(jnp.float32)).astype(jnp.bfloat16)

        @pl.loop(1, chips)
        def _(k):
            pltpu.make_async_remote_copy(
                src_ref=comb.at[g, k],
                dst_ref=recv.at[g, k],
                send_sem=scatter_sem.at[0, g],
                recv_sem=scatter_sem.at[1, g],
                device_id=peer((me + chips - k) % chips),
                device_id_type=MESH,
            ).start()

    def row_block(g, j):
        cut = pl.ds(j * 64, 64)
        q = q_scr[g, cut].reshape(wide, head_dim)
        do = do_scr[g, cut].reshape(wide, head_dim)
        return q, do, rows_ref[g, j, 0:1, :], rows_ref[g, j, 1:2, :]

    def branch_part(g):
        k_all = bk_ref[g]
        v_all = bv_ref[g]
        k_t_all = k_all.T
        steps = seq_len // 64
        for j in reversed(range(steps)):
            seen = (j + 1) * 64
            q, do, lse, delta = row_block(g, j)
            key_at = lax.broadcasted_iota(jnp.int32, (seen, wide), 0)
            row_at = lax.broadcasted_iota(jnp.int32, (seen, wide), 1) // group_size
            dq_t, dk, dv = block_terms(
                q, do, lse, delta, k_all[:seen], v_all[:seen], k_t_all[:, :seen],
                key_at <= row_at + j * 64, score_scale,
            )
            dq_acc[g, j] += dq_t
            if j == steps - 1:
                dk_acc[0:seen] = dk
                dv_acc[0:seen] = dv
            else:
                dk_acc[0:seen] += dk
                dv_acc[0:seen] += dv
        bdk_ref[g] = (dk_acc[0:seq_len] * scaling).astype(jnp.bfloat16)
        bdv_ref[g] = dv_acc[0:seq_len].astype(jnp.bfloat16)

    def prompt_part(g):
        kt_scr[...] = gath[g, :, :, 0].reshape(prompt_len, head_dim).T
        dk_acc[...] = jnp.zeros_like(dk_acc)
        dv_acc[...] = jnp.zeros_like(dv_acc)

        @pl.loop(0, seq_len // 64)
        def _(j):
            q, do, lse, delta = row_block(g, j)
            total = None
            for c in range(prompt_len // chunk):
                at = slice(c * chunk, (c + 1) * chunk)
                k = gath[g, c, :, 0].reshape(chunk, head_dim)
                v = gath[g, c, :, 1].reshape(chunk, head_dim)
                dq_t, dk, dv = block_terms(
                    q, do, lse, delta, k, v, kt_scr[:, at], None, score_scale
                )
                dk_acc[at] += dk
                dv_acc[at] += dv
                total = dq_t if total is None else total + dq_t
            dq_acc[g, j] += total

        own_part[g, :, 0] = (dk_acc[0:chunk] * scaling).reshape(chips, pos, head_dim)
        own_part[g, :, 1] = dv_acc[0:chunk].reshape(chips, pos, head_dim)
        send[g, :, 0] = (
            (dk_acc[chunk:] * scaling).astype(jnp.bfloat16).reshape(chips, pos, head_dim)
        )
        send[g, :, 1] = dv_acc[chunk:].astype(jnp.bfloat16).reshape(chips, pos, head_dim)
        half_copy(g).start()

    def store(g):
        cut = pl.ds(g * group_size, group_size)
        return pltpu.make_async_copy(dq_scr.at[g], dq_hbm.at[0, :, cut, :], store_sem.at[g])

    def finish(g):
        for j in range(seq_len // 64):
            dq_scr[g, j * 64 : (j + 1) * 64] = (
                (dq_acc[g, j] * scaling).T.astype(jnp.bfloat16).reshape(64, group_size, head_dim)
            )
        store(g).start()

    @pl.loop(0, early)
    def _(g):
        for copy in loads(g):
            copy.wait()
        branch_part(g)
        pass_on(g)

    @pl.loop(0, groups)
    def _(g):
        @pl.when(g >= early)
        def _():
            for copy in loads(g):
                copy.wait()

        pass_copy(g).wait_recv()
        prompt_part(g)

        @pl.when(g + early < groups)
        def _():
            pass_on(g + early)

        @pl.when(g > 0)
        def _():
            combine(g - 1)

    @pl.loop(0, early)
    def _(g):
        finish(g)

    combine(groups - 1)

    @pl.loop(early, groups)
    def _(g):
        branch_part(g)
        finish(g)

    @pl.loop(0, groups)
    def _(g):
        wait_bytes(gath.at[g, 0, far], gather_sem.at[0, g])
        pass_copy(g).wait_send()
        half_copy(g).wait_send()
        wait_bytes(comb.at[g, far], scatter_sem.at[0, g])
        wait_bytes(recv.at[g, far], scatter_sem.at[1, g])
        for apart in range(head_devices):
            owner = (me + apart) % head_devices
            total = None
            for k in range(apart, chips, head_devices):
                piece = (comb if k == 0 else recv)[g, k].astype(jnp.float32)
                total = piece if total is None else total + piece
            pd_ref[owner, g] = total.astype(jnp.bfloat16)
        store(g).wait()


def shards(
    queries,
    grad_out,
    branch_keys,
    branch_values,
    row_lse,
    row_delta,
    lengths,
    prompt_keys,
    prompt_values,
):
    branch_count = lax.axis_size("branch")
    head_devices = lax.axis_size("head")
    devices = branch_count * head_devices
    _, seq_len, head_count, head_dim = queries.shape
    groups = branch_keys.shape[2]
    group_size = head_count // groups
    pos = prompt_keys.shape[0]
    if pos % 16 or branch_count % 2:
        return plain_shards(
            queries, grad_out, branch_keys, branch_values, row_lse, row_delta, lengths,
            prompt_keys, prompt_values,
        )
    chips = devices // 2
    prompt_len = devices * pos
    wide = 64 * group_size
    steps = seq_len // 64
    live = lax.iota(jnp.int32, seq_len) < lengths[0]
    lse = jnp.where(live, row_lse[0] * LOG2E, 1e30)
    rows = jnp.stack([lse, row_delta[0]])
    rows = rows.reshape(2, groups, group_size, steps, 64)
    rows = rows.transpose(1, 3, 0, 4, 2).reshape(groups, steps, 2, wide)
    packed = jnp.stack([prompt_keys, prompt_values])
    packed = packed.reshape(2, pos, head_devices, groups, head_dim).transpose(2, 3, 0, 1, 4)
    dims = (branch_count, head_devices, groups, group_size, seq_len, head_dim, pos)
    vmem = pl.BlockSpec(memory_space=pltpu.VMEM)
    hbm = pl.BlockSpec(memory_space=pl.ANY)
    low, full = jnp.bfloat16, jnp.float32
    dq, bdk, bdv, pd = pl.pallas_call(
        functools.partial(fused_kernel, dims),
        out_shape=(
            jax.ShapeDtypeStruct(queries.shape, low),
            jax.ShapeDtypeStruct((groups, seq_len, head_dim), low),
            jax.ShapeDtypeStruct((groups, seq_len, head_dim), low),
            jax.ShapeDtypeStruct((head_devices, groups, 2, pos, head_dim), low),
        ),
        in_specs=[hbm, hbm, vmem, vmem, vmem, vmem],
        out_specs=(hbm, vmem, vmem, vmem),
        scratch_shapes=[
            pltpu.VMEM((groups, seq_len, group_size, head_dim), low),
            pltpu.VMEM((groups, seq_len, group_size, head_dim), low),
            pltpu.VMEM((groups, steps, head_dim, wide), full),
            pltpu.VMEM((groups, seq_len, group_size, head_dim), low),
            pltpu.VMEM((prompt_len, head_dim), full),
            pltpu.VMEM((prompt_len, head_dim), full),
            pltpu.VMEM((head_dim, prompt_len), low),
            pltpu.VMEM((groups, 2, chips, 2, pos, head_dim), low),
            pltpu.VMEM((groups, chips, 2, pos, head_dim), full),
            pltpu.VMEM((groups, chips, 2, pos, head_dim), low),
            pltpu.VMEM((groups, chips, 2, pos, head_dim), low),
            pltpu.VMEM((groups, chips, 2, pos, head_dim), low),
            pltpu.VMEM((groups, chips, 2, pos, head_dim), low),
            pltpu.SemaphoreType.DMA((2, groups)),
            pltpu.SemaphoreType.DMA((groups,)),
            pltpu.SemaphoreType.DMA((groups,)),
            pltpu.SemaphoreType.DMA((2, groups)),
            pltpu.SemaphoreType.DMA((2, groups)),
            pltpu.SemaphoreType.DMA((2, groups)),
            pltpu.SemaphoreType.DMA((2, groups)),
        ],
        compiler_params=pltpu.CompilerParams(collective_id=0, has_side_effects=True),
    )(
        queries,
        grad_out,
        branch_keys[0].swapaxes(0, 1),
        branch_values[0].swapaxes(0, 1),
        rows,
        packed,
    )
    pd = pd.transpose(2, 3, 0, 1, 4).reshape(2, pos, head_devices * groups, head_dim)
    return (dq, bdk.swapaxes(0, 1)[None], bdv.swapaxes(0, 1)[None], pd[0], pd[1])


def solution(mesh):
    in_specs = (
        P("branch", None, "head", None),
        P("branch", None, "head", None),
        P("branch", None, "head", None),
        P("branch", None, "head", None),
        P("branch", "head", None),
        P("branch", "head", None),
        P("branch"),
        P(("branch", "head"), None, None),
        P(("branch", "head"), None, None),
    )
    out_specs = (
        P("branch", None, "head", None),
        P("branch", None, "head", None),
        P("branch", None, "head", None),
        P(("branch", "head"), None, None),
        P(("branch", "head"), None, None),
    )
    return jax.shard_map(shards, mesh=mesh, in_specs=in_specs, out_specs=out_specs, check_vma=False)
```
